32 devices in a mesh: parts: 2 (over y), view: 4 (over x, core), tile: 4 (over z).
Axes of the slice: x: 2, y: 2, z: 4, core: 2. Of those that a mesh axis runs over, the one named last changes fastest.
Arguments:
- data: float32 [8, 32, 48, 32], P(('parts', 'view'), 'tile'), parts along dimension 0, may hold values from 0.25 to 4
- labels: int32 [8, 32, 48, 32], P(('parts', 'view'), 'tile'), parts along dimension 0, may hold values from 0 to 3
- kernel: float32 [4, 32, 9], P('view'), may hold values from 0.1 to 1
- offsets: int32 [4, 32], P('view'), may hold values from -2 to 2
Outputs:
- estimate: float32 [8, 32, 48, 32], P(('parts', 'view'), 'tile'), parts along dimension 0
The draws below stay inside these ranges and needn't reach their ends.
There are 2 independent parts, one for each index of `parts`. The reference program is written for one: setup_inputs(seed, part) draws one part's arguments, and reference() takes and returns one part's arrays. A program takes and returns all parts, laid end to end along the dimension named above; an argument that names none is the same for every part. Nothing has to cross between parts.
All inputs are finite; a program needn't handle non-finite values.
Results may differ from the reference program's by a relative error of at most 0.000088.
Values sent between devices are 32-bit elements; how exact they have to be, the bound alone decides.
A program may use at most 64 MiB of HBM per device.

```python
import math
import jax
import jax.numpy as jnp
from jax import lax

Y = 48
ITERS = 2
SWEEPS = 4
TAPS = 9
VIEWS = 4
X = 32
Z = 32


def plant(array, rng, smallest, top_value):
    shape = array.shape
    index_at = [jax.random.randint(jax.random.fold_in(rng, axis), (), 0, shape[axis]) for axis in range(len(shape))]
    array = array.at[tuple(index_at)].set(smallest)
    longest = shape.index(max(shape))
    index_at[longest] = (index_at[longest] + 1) % shape[longest]
    return array.at[tuple(index_at)].set(top_value)


def block_scale(own_key, extent, cuts, smallest, top_value):
    def one(dim, blocks):
        draws = jax.random.uniform(jax.random.fold_in(jax.random.fold_in(own_key, 6), dim), (blocks,), jnp.float32, smallest / len(cuts), top_value / len(cuts))
        return jnp.repeat(jnp.exp(draws), extent[dim] // blocks).reshape((-1,) + (1,) * (len(extent) - dim - 1))

    level = one(*cuts[0])
    for cut in cuts[1:]:
        level = level * one(*cut)
    return level


def setup_inputs(seed: int = 0, part: int = 0) -> dict:
    key_list = jax.random.split(jax.random.key(seed), 5)
    part_splits = jax.random.split(jax.random.fold_in(key_list[4], part), 5)
    return {
        "data": jnp.clip(jnp.exp(math.log(4.0) - 2.7725887 * jax.random.uniform(part_splits[0], (VIEWS, X, Y, Z), jnp.float32) ** block_scale(part_splits[0], (VIEWS, X, Y, Z), ((0, 4), (1, 4)), -0.2, 0.2)), 0.25, 4.0),
        "labels": plant(jax.random.randint(part_splits[1], (VIEWS, X, Y, Z), 0, 4), jax.random.fold_in(part_splits[1], 1), 0, 3).astype(jnp.int32),
        "kernel": jnp.clip(jnp.exp(math.log(1.0) - 2.3025851 * jax.random.uniform(key_list[2], (VIEWS, Z, TAPS), jnp.float32) ** block_scale(key_list[2], (VIEWS, Z, TAPS), ((0, 4),), -0.2, 0.2)), 0.1, 1.0),
        "offsets": plant(jax.random.randint(key_list[3], (VIEWS, Z), -2, 3), jax.random.fold_in(key_list[3], 1), -2, 2).astype(jnp.int32),
    }


WEAK = 0.2
TAU = 0.15

def band(kernel, offsets):
    depth_cells = kernel.shape[0]
    taps = jnp.arange(kernel.shape[1], dtype=jnp.int32) - 4
    depth = jnp.arange(depth_cells, dtype=jnp.int32)
    index = jnp.clip(depth[:, None] + taps[None, :] + offsets[:, None], 0, depth_cells - 1).astype(jnp.int32)
    weight = kernel / lax.optimization_barrier(jnp.sum(kernel, axis=1, keepdims=True))
    return (index, weight)

def blur_taps(field, index, weight):
    total = jnp.zeros_like(field)
    for k in range(index.shape[1]):
        total = total + jnp.take(field, index[:, k], axis=2) * weight[:, k]
    return total

def adjoint_taps(ratio, index, weight):
    total = jnp.zeros_like(ratio)
    for k in range(index.shape[1]):
        total = total.at[:, :, index[:, k]].add(ratio * weight[:, k])
    return total

def axis_term(field, region, axis):
    count = field.shape[axis]
    upper = lax.slice_in_dim(field, 1, count, axis=axis)
    lower = lax.slice_in_dim(field, 0, count - 1, axis=axis)
    same = jnp.where(lax.slice_in_dim(region, 1, count, axis=axis) == lax.slice_in_dim(region, 0, count - 1, axis=axis), 1.0, WEAK)
    flux = same * (upper - lower)
    after = [(0, 0)] * 3
    before = [(0, 0)] * 3
    after[axis] = (0, 1)
    before[axis] = (1, 0)
    return jnp.pad(flux, after) - jnp.pad(flux, before)

def sweep_whole(field, region):
    total = axis_term(field, region, 0) + axis_term(field, region, 1) + axis_term(field, region, 2)
    return field + TAU * total

def reference(data, labels, kernel, offsets):
    bands = [band(kernel[v], offsets[v]) for v in range(VIEWS)]
    current = [data[v] for v in range(VIEWS)]
    for step in range(ITERS):
        correction = [adjoint_taps(data[v] / blur_taps(current[v], *bands[v]), *bands[v]) for v in range(VIEWS)]
        paired = [jnp.sqrt(correction[v] * jnp.rot90(correction[(v + 2) % 4], 2, axes=(0, 2))) for v in range(VIEWS)]
        joined = [jnp.sqrt(paired[v] * jnp.rot90(paired[v ^ 1], 3 if v % 2 == 0 else 1, axes=(0, 2))) for v in range(VIEWS)]
        current = [current[v] * joined[v] for v in range(VIEWS)]
        for sweep in range(SWEEPS):
            current = [sweep_whole(current[v], labels[v]) for v in range(VIEWS)]
    return jnp.stack(current)
```

```python
import functools

import jax
import jax.numpy as jnp
from jax import lax
from jax.experimental import pallas as pl
from jax.experimental.pallas import tpu as pltpu
from jax.sharding import PartitionSpec as P

ITERS = 2
SWEEPS = 4


WEAK = 0.2
TAU = 0.15


def extended(cells, sides, width):
    for axis, dim in sides:
        count = lax.axis_size(axis)
        ends = count - 1
        head = lax.slice_in_dim(cells, 0, width, axis=dim)
        tail = lax.slice_in_dim(cells, cells.shape[dim] - width, cells.shape[dim], axis=dim)
        cells = jnp.concatenate(
            [
                lax.ppermute(tail, axis, [(i, (i + 1) % count) for i in range(ends)]),
                cells,
                lax.ppermute(head, axis, [((i + 1) % count, i) for i in range(ends)]),
            ],
            axis=dim,
        )
    return cells


def swapped(block, axis, stride):
    count = lax.axis_size(axis)
    route = []
    for low in range(count):
        high = low | 1 << stride
        if high != low and high < count:
            route += [(low, high), (high, low)]
    return lax.ppermute(block, axis, route)


def band(kernel, offsets):
    depth_cells = kernel.shape[0]
    taps = jnp.arange(kernel.shape[1], dtype=jnp.int32) - 4
    depth = jnp.arange(depth_cells, dtype=jnp.int32)
    index = jnp.clip(depth[:, None] + taps[None, :] + offsets[:, None], 0, depth_cells - 1)
    weight = kernel / jnp.sum(kernel, axis=1, keepdims=True)
    return (index, weight)


def axis_term(field, region, axis):
    count = field.shape[axis]
    upper = lax.slice_in_dim(field, 1, count, axis=axis)
    lower = lax.slice_in_dim(field, 0, count - 1, axis=axis)
    same = jnp.where(
        lax.slice_in_dim(region, 1, count, axis=axis)
        == lax.slice_in_dim(region, 0, count - 1, axis=axis),
        1.0,
        WEAK,
    )
    flux = same * (upper - lower)
    after = [(0, 0)] * 3
    before = [(0, 0)] * 3
    after[axis] = (0, 1)
    before[axis] = (1, 0)
    return jnp.pad(flux, after) - jnp.pad(flux, before)


def sweep_rows(field, region, first_row, total_rows):
    extent = field.shape[0]
    global_rows = first_row + jnp.arange(extent, dtype=jnp.int32)
    inside = ((global_rows >= 0) & (global_rows < total_rows)).astype(field.dtype)[:, None, None]
    same = jnp.where(region[1:] == region[:-1], 1.0, WEAK) * inside[1:] * inside[:-1]
    flux = same * (field[1:] - field[:-1])
    inner = field[1:-1]
    inner_labels = region[1:-1]
    total = (
        flux[1:] - flux[:-1] + axis_term(inner, inner_labels, 1) + axis_term(inner, inner_labels, 2)
    )
    return inner + TAU * total


def regroup(received, tiles):
    slab, rows, depth_cells = received.shape
    blocks = received.reshape(slab, rows, tiles, depth_cells // tiles)
    return blocks.transpose(3, 1, 2, 0).reshape(depth_cells // tiles, rows, depth_cells)


def on_device(data, labels, kernel, offsets):
    recorded = data[0]
    region = labels[0]
    index, weight = band(kernel[0], offsets[0])
    tiles = lax.axis_size("tile")
    slab, rows, depth_cells = recorded.shape
    total_rows = slab * tiles
    start = lax.axis_index("tile") * slab
    parity = lax.axis_index("view") % 2
    columns = jnp.arange(depth_cells, dtype=jnp.int32)
    matrix = jnp.sum(weight[:, :, None] * (index[:, :, None] == columns[None, None, :]), axis=1)
    label_ext = extended(region, (("tile", 0),), 4)
    current = recorded
    for step in range(ITERS):
        forward_flat = jnp.dot(
            current.reshape(-1, depth_cells), matrix.T, precision=lax.Precision.HIGHEST
        )
        field = recorded / forward_flat.reshape(current.shape)
        flat = jnp.dot(field.reshape(-1, depth_cells), matrix, precision=lax.Precision.HIGHEST)
        correction = flat.reshape(field.shape)
        turned = correction
        for repeat in range(2):
            turned = regroup(
                lax.all_to_all(
                    jnp.flip(turned, 2), "tile", split_axis=2, concat_axis=2, tiled=True
                ),
                tiles,
            )
        turned = swapped(turned, "view", 1)
        paired = jnp.sqrt(correction * turned)
        outgoing = jnp.where(parity == 0, jnp.flip(paired, 2), paired)
        rotated = regroup(
            lax.all_to_all(outgoing, "tile", split_axis=2, concat_axis=2, tiled=True), tiles
        )
        rotated = jnp.where(parity == 1, jnp.flip(rotated, 2), rotated)
        partner = swapped(rotated, "view", 0)
        current = current * jnp.sqrt(paired * partner)
        widened = extended(current, (("tile", 0),), 4)
        for sweep in range(SWEEPS):
            extent = widened.shape[0]
            widened = sweep_rows(
                widened, label_ext[sweep : sweep + extent], start - 4 + sweep, total_rows
            )
        current = widened
    return current[None]


def fused(tiles, data_ref, labels_ref, taps_ref, shift_ref, out_ref, raw, raw_labels, taps_buf, shift_buf, packed, packed_labels, held, held_labels, mats, est, coef, outgoing, incoming, halo, back, unpacked, in_sem, send, recv, send_l, recv_l, send_m, recv_m, send_p, recv_p, send_h, recv_h, send_o, recv_o, out_sem):
    mesh_id = pl.DeviceIdType.MESH
    slab, rows, depth = data_ref.shape[1:]
    lanes = packed.shape[2]
    fold = lanes // depth
    groups = rows // fold
    per_tile = groups // tiles
    width = held.shape[1]
    cells = held.shape[2]
    peers = 2 * tiles
    view = lax.axis_index("view")
    tile = lax.axis_index("tile")
    part = lax.axis_index("parts")
    half = view // 2
    core = view % 2
    me = half * tiles + tile
    flip_x = (view == 1) | (view == 2)
    flip_z = view >= 2

    def peer(q):
        return (part, 2 * (q // tiles) + core, q % tiles)

    copies_in = []
    for source, target, base in ((data_ref, raw, 0), (labels_ref, raw_labels, slab)):
        for x in range(slab):
            at = jnp.where(flip_x, slab - 1 - x, x)
            copies_in.append(
                pltpu.make_async_copy(
                    source.at[0, x],
                    target.at[pl.ds(pl.multiple_of(at * rows, 8), rows)],
                    in_sem.at[base + x],
                )
            )
    copies_in.append(pltpu.make_async_copy(taps_ref.at[0], taps_buf, in_sem.at[2 * slab]))
    copies_in.append(pltpu.make_async_copy(shift_ref, shift_buf, in_sem.at[2 * slab + 1]))
    for copy in copies_in:
        copy.start()

    barrier = pltpu.get_barrier_semaphore()
    across = (part, 2 * half + 1 - core, tile)
    for d in range(1, peers):
        pl.semaphore_signal(barrier, inc=1, device_id=peer((me + d) % peers), device_id_type=mesh_id)
    pl.semaphore_signal(barrier, inc=1, device_id=across, device_id_type=mesh_id)

    row_ids = lax.broadcasted_iota(jnp.int32, (lanes, lanes), 0)
    lane_ids = lax.broadcasted_iota(jnp.int32, (lanes, lanes), 1)
    same_block = (row_ids // depth) == (lane_ids // depth)
    aim = jnp.where(flip_z, depth - 1 - lane_ids % depth, lane_ids % depth)
    turn = jnp.where(same_block & (row_ids % depth == aim), 1.0, 0.0).astype(jnp.float32)

    def exact(a, b):
        return jnp.dot(a, b, precision=lax.Precision.HIGHEST, preferred_element_type=jnp.float32)

    def pack(source, target, fill, convert):
        pieces = []
        for g in range(groups):
            pieces.append(
                jnp.concatenate(
                    [convert(source[pl.ds(g * fold + b, slab, stride=rows), :]) for b in range(fold)],
                    axis=1,
                )
            )
        turned = exact(jnp.concatenate(pieces, axis=0), turn)
        edge = jnp.full((1, slab, lanes), fill, jnp.float32)
        target[0:1] = edge
        target[groups + 1 : groups + 2] = edge
        target[1 : groups + 1] = turned.reshape(groups, slab, lanes)

    spot = pl.ds(pl.multiple_of(jnp.where(flip_x, tiles - 1 - tile, tile) * slab, 8), slab)

    def scatter(source, target, send_sem, recv_sem):
        copies = []
        for d in range(peers):
            q = (me + d) % peers
            src = source.at[pl.ds(per_tile * (q % tiles) + q // tiles, width)]
            dst = target.at[half, :, spot, :]
            if d == 0:
                copy = pltpu.make_async_copy(src, dst, recv_sem.at[0])
            else:
                copy = pltpu.make_async_remote_copy(
                    src_ref=src,
                    dst_ref=dst,
                    send_sem=send_sem.at[d],
                    recv_sem=recv_sem.at[d],
                    device_id=peer(q),
                    device_id_type=mesh_id,
                )
            copy.start()
            copies.append(copy)
        return copies

    def landed(copies):
        copies[0].wait()
        for copy in copies[1:]:
            copy.wait_recv()

    for x in range(slab):
        copies_in[x].wait()
    pack(raw, packed, 1.0, lambda v: v)
    pl.semaphore_wait(barrier, peers)
    data_copies = scatter(packed, held, send, recv)

    copies_in[2 * slab].wait()
    copies_in[2 * slab + 1].wait()
    taps = taps_buf[...]
    count = taps.shape[1]
    weight = taps / jnp.sum(taps, axis=1, keepdims=True)
    shift_row = jnp.broadcast_to(shift_buf[...].astype(jnp.float32), (depth, depth))
    eye = lax.broadcasted_iota(jnp.int32, (depth, depth), 0) == lax.broadcasted_iota(
        jnp.int32, (depth, depth), 1
    )
    shift = jnp.sum(jnp.where(eye, shift_row, 0.0), axis=1, keepdims=True).astype(jnp.int32)
    level = lax.broadcasted_iota(jnp.int32, (depth, 1), 0)
    strip_lane = lax.broadcasted_iota(jnp.int32, (depth, lanes), 1) % depth
    strip_aim = jnp.where(flip_z, depth - 1 - strip_lane, strip_lane)
    strip = jnp.zeros((depth, lanes), jnp.float32)
    for k in range(count):
        index = jnp.clip(level + (k - 4) + shift, 0, depth - 1)
        strip = strip + jnp.where(index == strip_aim, weight[:, k : k + 1], 0.0)
    strip = exact(turn[:depth, :depth], strip)
    mats[pl.ds(half, 1)] = strip[None]
    mat_copy = pltpu.make_async_remote_copy(
        src_ref=mats.at[half],
        dst_ref=mats.at[half],
        send_sem=send_m,
        recv_sem=recv_m,
        device_id=(part, 2 * (1 - half) + core, tile),
        device_id_type=mesh_id,
    )
    mat_copy.start()

    for x in range(slab):
        copies_in[slab + x].wait()
    pack(raw_labels, packed_labels, 0.0, lambda v: v.astype(jnp.float32))
    label_copies = scatter(packed_labels, held_labels, send_l, recv_l)

    lane = lax.broadcasted_iota(jnp.int32, (cells, lanes), 1)
    sub = lax.broadcasted_iota(jnp.int32, (cells, lanes), 0)
    first = per_tile * tile - 1 + half
    last_lane = lane < lanes - depth
    first_lane = lane < depth

    def ahead_y(fields, g):
        return jnp.where(
            last_lane,
            pltpu.roll(fields[g], lanes - depth, 1),
            pltpu.roll(fields[(g + 1) % width], lanes - depth, 1),
        )

    def behind_y(fields, g):
        return jnp.where(
            first_lane,
            pltpu.roll(fields[(g - 1) % width], depth, 1),
            pltpu.roll(fields[g], depth, 1),
        )

    def transposed(p):
        flipped = p.T
        result = []
        for g in range(width):
            piece = flipped[0:depth]
            if g:
                piece = pltpu.roll(piece, (lanes - depth * g) % lanes, 1)
            for b in range(1, fold):
                part_b = flipped[depth * b : depth * (b + 1)]
                amount = (depth * (b - g)) % lanes
                if amount:
                    part_b = pltpu.roll(part_b, amount, 1)
                piece = jnp.where(lane // depth == b, part_b, piece)
            result.append(piece)
        return result

    landed(data_copies)
    mat_copy.wait_recv()
    blurs = [
        jnp.where(same_block, jnp.concatenate([mats[s]] * fold, axis=0), 0.0) for s in range(2)
    ]

    pending = []
    for step in range(ITERS):
        corrections = []
        for s in range(2):
            recorded = held[s].reshape(width * cells, lanes)
            current = recorded if step == 0 else est[s].reshape(width * cells, lanes)
            forward = lax.dot_general(
                current,
                blurs[s],
                (((1,), (1,)), ((), ())),
                precision=lax.Precision.HIGHEST,
                preferred_element_type=jnp.float32,
            )
            corrections.append(exact(recorded / forward, blurs[s]))
        paired = jnp.sqrt(corrections[0] * corrections[1])
        pieces = transposed(paired)
        for g in range(width):
            outgoing[step, g] = pieces[g]
        swap = pltpu.make_async_remote_copy(
            src_ref=outgoing.at[step],
            dst_ref=incoming.at[step],
            send_sem=send_p.at[step],
            recv_sem=recv_p.at[step],
            device_id=across,
            device_id_type=mesh_id,
        )
        swap.start()
        pending.append(swap)
        if step == 0:
            landed(label_copies)
            for s in range(2):
                regions = [held_labels[s, g] for g in range(width)]
                for g in range(width):
                    mine = regions[g]
                    strong, weak = TAU, TAU * WEAK
                    e_x = jnp.where(pltpu.roll(mine, cells - 1, 0) == mine, strong, weak)
                    coef[0, s, g] = jnp.where(sub == cells - 1, 0.0, e_x)
                    e_z = jnp.where(pltpu.roll(mine, lanes - 1, 1) == mine, strong, weak)
                    coef[1, s, g] = jnp.where(lane % depth == depth - 1, 0.0, e_z)
                    e_y = jnp.where(ahead_y(regions, g) == mine, strong, weak)
                    y = fold * (first + g) + lane // depth
                    coef[2, s, g] = jnp.where((y >= 0) & (y < rows - 1), e_y, 0.0)
        swap.wait_recv()
        joined = [
            jnp.sqrt(paired[cells * g : cells * (g + 1)] * incoming[step, g]) for g in range(width)
        ]
        for s in range(2):
            base = held if step == 0 else est
            fields = [base[s, g] * joined[g] for g in range(width)]
            for sweep in range(SWEEPS):
                flux_y = [coef[2, s, g] * (ahead_y(fields, g) - fields[g]) for g in range(width)]
                fresh = []
                for g in range(width):
                    f = fields[g]
                    flux_x = coef[0, s, g] * (pltpu.roll(f, cells - 1, 0) - f)
                    flux_z = coef[1, s, g] * (pltpu.roll(f, lanes - 1, 1) - f)
                    total = (
                        (flux_x - pltpu.roll(flux_x, 1, 0))
                        + (flux_y[g] - behind_y(flux_y, g))
                        + (flux_z - pltpu.roll(flux_z, 1, 1))
                    )
                    fresh.append(f + total)
                fields = fresh
            for g in range(width):
                est[s, g] = fields[g]
        if step < ITERS - 1:
            far = tile + 2 * half - 1
            exists = (far >= 0) & (far < tiles)

            def shifted(number, side, target):
                return pltpu.make_async_remote_copy(
                    src_ref=est.at[:, 1 + half],
                    dst_ref=halo.at[step, side],
                    send_sem=send_h.at[step, number],
                    recv_sem=recv_h.at[step, number],
                    device_id=(part, 2 * (1 - half) + core, target),
                    device_id_type=mesh_id,
                )

            near_copy = shifted(0, half, tile)
            near_copy.start()
            far_copy = shifted(1, 1 - half, jnp.clip(far, 0, tiles - 1))

            @pl.when(exists)
            def _():
                far_copy.start()

            near_copy.wait()
            near = (width - 1) * (1 - half)
            for s in range(2):
                est[s, pl.ds(near, 1)] = halo[step, 1 - half, s][None]

            @pl.when(exists)
            def _():
                far_copy.wait()
                for s in range(2):
                    est[s, pl.ds((width - 1) * half, 1)] = halo[step, half, s][None]

    out_copies = []
    for d in range(peers):
        q = (me + d) % peers
        s, t = q // tiles, q % tiles
        place = jnp.where(s + core == 1, tiles - 1 - t, t)
        src = est.at[s, 1 : width - 1, pl.ds(pl.multiple_of(place * slab, 8), slab), :]
        dst = back.at[me]
        if d == 0:
            copy = pltpu.make_async_copy(src, dst, recv_o.at[0])
        else:
            copy = pltpu.make_async_remote_copy(
                src_ref=src,
                dst_ref=dst,
                send_sem=send_o.at[d],
                recv_sem=recv_o.at[d],
                device_id=peer(q),
                device_id_type=mesh_id,
            )
        copy.start()
        out_copies.append(copy)
    landed(out_copies)
    pieces = []
    for g in range(groups):
        m, r = g // per_tile, g % per_tile
        pieces.append(back[m, r] if r < 2 else back[tiles + m, r - 1])
    turned = exact(jnp.concatenate(pieces, axis=0), turn)
    for g in range(groups):
        for b in range(fold):
            unpacked[pl.ds(g * fold + b, slab, stride=rows), :] = turned[
                g * slab : (g + 1) * slab, b * depth : (b + 1) * depth
            ]
    results = []
    for x in range(slab):
        at = jnp.where(flip_x, slab - 1 - x, x)
        copy = pltpu.make_async_copy(
            unpacked.at[pl.ds(pl.multiple_of(at * rows, 8), rows)], out_ref.at[0, x], out_sem.at[x]
        )
        copy.start()
        results.append(copy)
    for copy in data_copies[1:] + label_copies[1:] + [mat_copy] + pending + out_copies[1:]:
        copy.wait_send()
    for copy in results:
        copy.wait()


def by_rows(data, labels, kernel, offsets):
    tiles = lax.axis_size("tile")
    _, slab, rows, depth = data.shape
    fold = 128 // depth
    groups = rows // fold
    cells = slab * tiles
    peers = 2 * tiles
    width = 4
    flat = (slab * rows, depth)
    wide = (2, width, cells, 128)
    dma = pltpu.SemaphoreType.DMA
    return pl.pallas_call(
        functools.partial(fused, tiles),
        out_shape=jax.ShapeDtypeStruct(data.shape, jnp.float32),
        in_specs=[pl.BlockSpec(memory_space=pl.ANY)] * 4,
        out_specs=pl.BlockSpec(memory_space=pl.ANY),
        scratch_shapes=[
            pltpu.VMEM(flat, jnp.float32),
            pltpu.VMEM(flat, jnp.int32),
            pltpu.VMEM(kernel.shape[1:], jnp.float32),
            pltpu.VMEM(offsets.shape, jnp.int32),
            pltpu.VMEM((groups + 2, slab, 128), jnp.float32),
            pltpu.VMEM((groups + 2, slab, 128), jnp.float32),
            pltpu.VMEM(wide, jnp.float32),
            pltpu.VMEM(wide, jnp.float32),
            pltpu.VMEM((2, depth, 128), jnp.float32),
            pltpu.VMEM(wide, jnp.float32),
            pltpu.VMEM((3,) + wide, jnp.float32),
            pltpu.VMEM((ITERS,) + wide[1:], jnp.float32),
            pltpu.VMEM((ITERS,) + wide[1:], jnp.float32),
            pltpu.VMEM((ITERS - 1, 2, 2, cells, 128), jnp.float32),
            pltpu.VMEM((peers, width - 2, slab, 128), jnp.float32),
            pltpu.VMEM(flat, jnp.float32),
            dma((2 * slab + 2,)),
            dma((peers,)),
            dma((peers,)),
            dma((peers,)),
            dma((peers,)),
            dma(()),
            dma(()),
            dma((ITERS,)),
            dma((ITERS,)),
            dma((ITERS - 1, 2)),
            dma((ITERS - 1, 2)),
            dma((peers,)),
            dma((peers,)),
            dma((slab,)),
        ],
        compiler_params=pltpu.CompilerParams(collective_id=0, has_side_effects=True),
    )(data, labels, kernel, offsets)


def fits(data, tiles, views):
    _, slab, rows, depth = data.shape
    return (
        views == 4
        and depth * 4 == 128
        and slab * tiles == depth
        and slab % 8 == 0
        and rows == 12 * tiles
    )


def program(data, labels, kernel, offsets):
    if fits(data, lax.axis_size("tile"), lax.axis_size("view")):
        return by_rows(data, labels, kernel, offsets)
    return on_device(data, labels, kernel, offsets)


def solution(mesh):
    placed = (
        P(("parts", "view"), "tile", None, None),
        P(("parts", "view"), "tile", None, None),
        P("view", None, None),
        P("view", None),
    )
    return jax.shard_map(
        program,
        mesh=mesh,
        in_specs=placed,
        out_specs=P(("parts", "view"), "tile", None, None),
        check_vma=False,
    )
```

```python
import functools

import jax
import jax.numpy as jnp
from jax import lax
from jax.experimental import pallas as pl
from jax.experimental.pallas import tpu as pltpu
from jax.sharding import PartitionSpec as P

ITERS = 2
SWEEPS = 4


WEAK = 0.2
TAU = 0.15


def extended(cells, sides, width):
    for axis, dim in sides:
        count = lax.axis_size(axis)
        ends = count - 1
        head = lax.slice_in_dim(cells, 0, width, axis=dim)
        tail = lax.slice_in_dim(cells, cells.shape[dim] - width, cells.shape[dim], axis=dim)
        cells = jnp.concatenate(
            [
                lax.ppermute(tail, axis, [(i, (i + 1) % count) for i in range(ends)]),
                cells,
                lax.ppermute(head, axis, [((i + 1) % count, i) for i in range(ends)]),
            ],
            axis=dim,
        )
    return cells


def swapped(block, axis, stride):
    count = lax.axis_size(axis)
    route = []
    for low in range(count):
        high = low | 1 << stride
        if high != low and high < count:
            route += [(low, high), (high, low)]
    return lax.ppermute(block, axis, route)


def band(kernel, offsets):
    depth_cells = kernel.shape[0]
    taps = jnp.arange(kernel.shape[1], dtype=jnp.int32) - 4
    depth = jnp.arange(depth_cells, dtype=jnp.int32)
    index = jnp.clip(depth[:, None] + taps[None, :] + offsets[:, None], 0, depth_cells - 1)
    weight = kernel / jnp.sum(kernel, axis=1, keepdims=True)
    return (index, weight)


def axis_term(field, region, axis):
    count = field.shape[axis]
    upper = lax.slice_in_dim(field, 1, count, axis=axis)
    lower = lax.slice_in_dim(field, 0, count - 1, axis=axis)
    same = jnp.where(
        lax.slice_in_dim(region, 1, count, axis=axis)
        == lax.slice_in_dim(region, 0, count - 1, axis=axis),
        1.0,
        WEAK,
    )
    flux = same * (upper - lower)
    after = [(0, 0)] * 3
    before = [(0, 0)] * 3
    after[axis] = (0, 1)
    before[axis] = (1, 0)
    return jnp.pad(flux, after) - jnp.pad(flux, before)


def sweep_rows(field, region, first_row, total_rows):
    extent = field.shape[0]
    global_rows = first_row + jnp.arange(extent, dtype=jnp.int32)
    inside = ((global_rows >= 0) & (global_rows < total_rows)).astype(field.dtype)[:, None, None]
    same = jnp.where(region[1:] == region[:-1], 1.0, WEAK) * inside[1:] * inside[:-1]
    flux = same * (field[1:] - field[:-1])
    inner = field[1:-1]
    inner_labels = region[1:-1]
    total = (
        flux[1:] - flux[:-1] + axis_term(inner, inner_labels, 1) + axis_term(inner, inner_labels, 2)
    )
    return inner + TAU * total


def regroup(received, tiles):
    slab, rows, depth_cells = received.shape
    blocks = received.reshape(slab, rows, tiles, depth_cells // tiles)
    return blocks.transpose(3, 1, 2, 0).reshape(depth_cells // tiles, rows, depth_cells)


def on_device(data, labels, kernel, offsets):
    recorded = data[0]
    region = labels[0]
    index, weight = band(kernel[0], offsets[0])
    tiles = lax.axis_size("tile")
    slab, rows, depth_cells = recorded.shape
    total_rows = slab * tiles
    start = lax.axis_index("tile") * slab
    parity = lax.axis_index("view") % 2
    columns = jnp.arange(depth_cells, dtype=jnp.int32)
    matrix = jnp.sum(weight[:, :, None] * (index[:, :, None] == columns[None, None, :]), axis=1)
    label_ext = extended(region, (("tile", 0),), 4)
    current = recorded
    for step in range(ITERS):
        forward_flat = jnp.dot(
            current.reshape(-1, depth_cells), matrix.T, precision=lax.Precision.HIGHEST
        )
        field = recorded / forward_flat.reshape(current.shape)
        flat = jnp.dot(field.reshape(-1, depth_cells), matrix, precision=lax.Precision.HIGHEST)
        correction = flat.reshape(field.shape)
        turned = correction
        for repeat in range(2):
            turned = regroup(
                lax.all_to_all(
                    jnp.flip(turned, 2), "tile", split_axis=2, concat_axis=2, tiled=True
                ),
                tiles,
            )
        turned = swapped(turned, "view", 1)
        paired = jnp.sqrt(correction * turned)
        outgoing = jnp.where(parity == 0, jnp.flip(paired, 2), paired)
        rotated = regroup(
            lax.all_to_all(outgoing, "tile", split_axis=2, concat_axis=2, tiled=True), tiles
        )
        rotated = jnp.where(parity == 1, jnp.flip(rotated, 2), rotated)
        partner = swapped(rotated, "view", 0)
        current = current * jnp.sqrt(paired * partner)
        widened = extended(current, (("tile", 0),), 4)
        for sweep in range(SWEEPS):
            extent = widened.shape[0]
            widened = sweep_rows(
                widened, label_ext[sweep : sweep + extent], start - 4 + sweep, total_rows
            )
        current = widened
    return current[None]


def fused(tiles, data_ref, labels_ref, taps_ref, shift_ref, out_ref, raw, raw_labels, taps_buf, shift_buf, mixed, packed, packed_labels, held, held_labels, mats, est, coef, outgoing, incoming, halo, back, unpacked, in_sem, send, recv, send_l, recv_l, send_m, recv_m, send_p, recv_p, send_h, recv_h, send_o, recv_o, out_sem):
    mesh_id = pl.DeviceIdType.MESH
    slab, depth, rows = data_ref.shape[1:]
    lanes = packed.shape[2]
    fold = lanes // depth
    groups = rows // fold
    per_tile = groups // tiles
    width = held.shape[1]
    cells = held.shape[2]
    peers = 2 * tiles
    view = lax.axis_index("view")
    tile = lax.axis_index("tile")
    part = lax.axis_index("parts")
    half = view // 2
    core = view % 2
    me = half * tiles + tile
    role = (half + tile) % 2
    flip_x = (view == 1) | (view == 2)
    flip_z = view >= 2

    def peer(q):
        return (part, 2 * (q // tiles) + core, q % tiles)

    copies_in = []
    for source, target, base in ((data_ref, raw, 0), (labels_ref, raw_labels, slab)):
        for x in range(slab):
            at = jnp.where(flip_x, slab - 1 - x, x)
            copies_in.append(
                pltpu.make_async_copy(
                    source.at[0, x],
                    target.at[pl.ds(pl.multiple_of(at * depth, 8), depth)],
                    in_sem.at[base + x],
                )
            )
    copies_in.append(pltpu.make_async_copy(taps_ref, taps_buf, in_sem.at[2 * slab]))
    copies_in.append(pltpu.make_async_copy(shift_ref, shift_buf, in_sem.at[2 * slab + 1]))
    for copy in copies_in:
        copy.start()

    barrier = pltpu.get_barrier_semaphore()
    across = (part, 2 * half + 1 - core, tile)
    for d in range(1, peers):
        pl.semaphore_signal(barrier, inc=1, device_id=peer((me + d) % peers), device_id_type=mesh_id)
    pl.semaphore_signal(barrier, inc=1, device_id=across, device_id_type=mesh_id)

    row_ids = lax.broadcasted_iota(jnp.int32, (lanes, lanes), 0)
    lane_ids = lax.broadcasted_iota(jnp.int32, (lanes, lanes), 1)
    same_block = (row_ids // depth) == (lane_ids // depth)
    aim = jnp.where(flip_z, depth - 1 - lane_ids % depth, lane_ids % depth)
    turn = jnp.where(same_block & (row_ids % depth == aim), 1.0, 0.0).astype(jnp.float32)

    def exact(a, b):
        return jnp.dot(a, b, precision=lax.Precision.HIGHEST, preferred_element_type=jnp.float32)

    slot = lax.broadcasted_iota(jnp.int32, (mixed.shape[1] // fold, lanes), 1) // depth
    blocks = slab * depth // lanes

    def gathered(parts, b_of):
        total = None
        for k in range(fold):
            amount = (depth * (k - b_of[k])) % lanes
            piece = pltpu.roll(parts[k], amount, 1) if amount else parts[k]
            total = piece if total is None else jnp.where(slot == k, piece, total)
        return total

    def pack(source, target, fill, convert):
        edge = jnp.full((1, slab, lanes), fill, jnp.float32)
        target[0:1] = edge
        target[groups + 1 : groups + 2] = edge
        for j in range(blocks):
            block = convert(source[lanes * j : lanes * (j + 1), :])
            mixed[j, 0:rows] = exact(block.T, turn)
        for j in range(blocks):
            parts = [
                mixed[j, pl.ds(b, mixed.shape[1] // fold, stride=fold), :] for b in range(fold)
            ]
            for k in range(fold):
                line = gathered(parts, [k] * fold)
                target[1 : groups + 1, fold * j + k, :] = line[:groups]

    spot = pl.ds(pl.multiple_of(jnp.where(flip_x, tiles - 1 - tile, tile) * slab, 8), slab)

    def scatter(source, target, send_sem, recv_sem):
        copies = []
        for d in range(peers):
            q = (me + d) % peers
            src = source.at[pl.ds(per_tile * (q % tiles) + (q // tiles + q % tiles) % 2, width)]
            dst = target.at[half, :, spot, :]
            if d == 0:
                copy = pltpu.make_async_copy(src, dst, recv_sem.at[0])
            else:
                copy = pltpu.make_async_remote_copy(
                    src_ref=src,
                    dst_ref=dst,
                    send_sem=send_sem.at[d],
                    recv_sem=recv_sem.at[d],
                    device_id=peer(q),
                    device_id_type=mesh_id,
                )
            copy.start()
            copies.append(copy)
        return copies

    def landed(copies):
        copies[0].wait()
        for copy in copies[1:]:
            copy.wait_recv()

    for x in range(slab):
        copies_in[x].wait()
    pack(raw, packed, 1.0, lambda v: v)
    pl.semaphore_wait(barrier, peers)
    data_copies = scatter(packed, held, send, recv)

    copies_in[2 * slab].wait()
    copies_in[2 * slab + 1].wait()
    count = taps_buf.shape[0]
    taps = [jnp.concatenate([taps_buf[k]] * fold, axis=1) for k in range(count)]
    scale = taps[0]
    for k in range(1, count):
        scale = scale + taps[k]
    shift = jnp.concatenate([shift_buf[...]] * fold, axis=1)
    level = lax.broadcasted_iota(jnp.int32, (1, lanes), 1) % depth
    strip_row = lax.broadcasted_iota(jnp.int32, (depth, lanes), 0)
    strip_aim = jnp.where(flip_z, depth - 1 - strip_row, strip_row)
    strip = jnp.zeros((depth, lanes), jnp.float32)
    for k in range(count):
        index = jnp.clip(level + (k - 4) + shift, 0, depth - 1)
        strip = strip + jnp.where(index == strip_aim, taps[k] / scale, 0.0)
    strip = exact(strip, turn)
    mats[pl.ds(half, 1)] = strip[None]
    mat_copy = pltpu.make_async_remote_copy(
        src_ref=mats.at[half],
        dst_ref=mats.at[half],
        send_sem=send_m,
        recv_sem=recv_m,
        device_id=(part, 2 * (1 - half) + core, tile),
        device_id_type=mesh_id,
    )
    mat_copy.start()

    for x in range(slab):
        copies_in[slab + x].wait()
    pack(raw_labels, packed_labels, 0.0, lambda v: v.astype(jnp.float32))
    label_copies = scatter(packed_labels, held_labels, send_l, recv_l)

    lane = lax.broadcasted_iota(jnp.int32, (cells, lanes), 1)
    sub = lax.broadcasted_iota(jnp.int32, (cells, lanes), 0)
    first = per_tile * tile - 1 + role
    last_lane = lane < lanes - depth
    first_lane = lane < depth

    def ahead_y(fields, g):
        return jnp.where(
            last_lane,
            pltpu.roll(fields[g], lanes - depth, 1),
            pltpu.roll(fields[(g + 1) % width], lanes - depth, 1),
        )

    def behind_y(fields, g):
        return jnp.where(
            first_lane,
            pltpu.roll(fields[(g - 1) % width], depth, 1),
            pltpu.roll(fields[g], depth, 1),
        )

    def transposed(p, chosen):
        flipped = p.T
        result = []
        for g in chosen:
            piece = flipped[0:depth]
            if g:
                piece = pltpu.roll(piece, (lanes - depth * g) % lanes, 1)
            for b in range(1, fold):
                part_b = flipped[depth * b : depth * (b + 1)]
                amount = (depth * (b - g)) % lanes
                if amount:
                    part_b = pltpu.roll(part_b, amount, 1)
                piece = jnp.where(lane // depth == b, part_b, piece)
            result.append(piece)
        return result

    landed(data_copies)
    mat_copy.wait_recv()
    blurs = [
        jnp.where(same_block, jnp.concatenate([mats[s]] * fold, axis=0), 0.0) for s in range(2)
    ]

    def paired_of(step, chosen):
        corrections = []
        for s in range(2):
            recorded = jnp.concatenate([held[s, g] for g in chosen], axis=0)
            if step == 0:
                current = recorded
            else:
                current = jnp.concatenate([est[s, g] for g in chosen], axis=0)
            ratio = recorded / exact(current, blurs[s])
            corrections.append(
                lax.dot_general(
                    ratio,
                    blurs[s],
                    (((1,), (1,)), ((), ())),
                    precision=lax.Precision.HIGHEST,
                    preferred_element_type=jnp.float32,
                )
            )
        return jnp.sqrt(corrections[0] * corrections[1])

    def swapped_over(step, number, begin, size):
        copy = pltpu.make_async_remote_copy(
            src_ref=outgoing.at[step, pl.ds(begin, size)],
            dst_ref=incoming.at[step, pl.ds(begin, size)],
            send_sem=send_p.at[step, number],
            recv_sem=recv_p.at[step, number],
            device_id=across,
            device_id_type=mesh_id,
        )
        copy.start()
        pending.append(copy)
        return copy

    pending = []
    ready = {}
    for step in range(ITERS):
        if step == 0:
            whole = paired_of(0, range(width))
            for g, piece in enumerate(transposed(whole, range(width))):
                outgoing[step, g] = piece
                ready[g] = whole[cells * g : cells * (g + 1)]
            swaps = [swapped_over(step, 0, 0, width)]
        else:
            inner = range(1, width - 1)
            outer = (0, width - 1)
            near_copy, far_copy, exists = moving
            swaps = []
            for number, chosen in enumerate((inner, outer)):
                if number:
                    near_copy.wait()
                    near = (width - 1) * (1 - role)
                    for s in range(2):
                        est[s, pl.ds(near, 1)] = halo[step - 1, 1 - role, s][None]

                    @pl.when(exists)
                    def _():
                        far_copy.wait()
                        for s in range(2):
                            est[s, pl.ds((width - 1) * role, 1)] = halo[step - 1, role, s][None]

                part_p = paired_of(step, chosen)
                turned_p = transposed(jnp.concatenate([part_p, part_p], axis=0), range(len(chosen)))
                for k, g in enumerate(chosen):
                    outgoing[step, g] = turned_p[k]
                    ready[g] = part_p[cells * k : cells * (k + 1)]
                if number:
                    swaps += [swapped_over(step, 1 + k, g, 1) for k, g in enumerate(chosen)]
                else:
                    swaps.append(swapped_over(step, 0, 1, width - 2))
        if step == 0:
            landed(label_copies)
            for s in range(2):
                regions = [held_labels[s, g] for g in range(width)]
                for g in range(width):
                    mine = regions[g]
                    strong, weak = TAU, TAU * WEAK
                    e_x = jnp.where(pltpu.roll(mine, cells - 1, 0) == mine, strong, weak)
                    coef[0, s, g] = jnp.where(sub == cells - 1, 0.0, e_x)
                    e_z = jnp.where(pltpu.roll(mine, lanes - 1, 1) == mine, strong, weak)
                    coef[1, s, g] = jnp.where(lane % depth == depth - 1, 0.0, e_z)
                    e_y = jnp.where(ahead_y(regions, g) == mine, strong, weak)
                    y = fold * (first + g) + lane // depth
                    coef[2, s, g] = jnp.where((y >= 0) & (y < rows - 1), e_y, 0.0)
        for swap in swaps:
            swap.wait_recv()
        joined = [jnp.sqrt(ready[g] * incoming[step, g]) for g in range(width)]
        for s in range(2):
            base = held if step == 0 else est
            fields = [base[s, g] * joined[g] for g in range(width)]
            for sweep in range(SWEEPS):
                flux_y = [coef[2, s, g] * (ahead_y(fields, g) - fields[g]) for g in range(width)]
                fresh = []
                for g in range(width):
                    f = fields[g]
                    flux_x = coef[0, s, g] * (pltpu.roll(f, cells - 1, 0) - f)
                    flux_z = coef[1, s, g] * (pltpu.roll(f, lanes - 1, 1) - f)
                    total = (
                        (flux_x - pltpu.roll(flux_x, 1, 0))
                        + (flux_y[g] - behind_y(flux_y, g))
                        + (flux_z - pltpu.roll(flux_z, 1, 1))
                    )
                    fresh.append(f + total)
                fields = fresh
            for g in range(width):
                est[s, g] = fields[g]
        if step < ITERS - 1:
            far = tile + 2 * role - 1
            exists = (far >= 0) & (far < tiles)

            def shifted(number, side, x_of, target):
                return pltpu.make_async_remote_copy(
                    src_ref=est.at[:, 1 + role],
                    dst_ref=halo.at[step, side],
                    send_sem=send_h.at[step, number],
                    recv_sem=recv_h.at[step, number],
                    device_id=(part, 2 * x_of + core, target),
                    device_id_type=mesh_id,
                )

            near_copy = shifted(0, role, 1 - half, tile)
            near_copy.start()
            far_copy = shifted(1, 1 - role, half, jnp.clip(far, 0, tiles - 1))

            @pl.when(exists)
            def _():
                far_copy.start()

            moving = (near_copy, far_copy, exists)

    out_copies = []
    for middle in range(2):
        for d in range(tiles if middle else peers):
            q = half * tiles + (tile + d) % tiles if middle else (me + d) % peers
            s, t = q // tiles, q % tiles
            place = jnp.where(s + core == 1, tiles - 1 - t, t)
            here = 2 - role if middle else 1 + role
            there = per_tile * tile + (1 if middle else 2 * role)
            src = est.at[s, here, pl.ds(pl.multiple_of(place * slab, 8), slab), :]
            dst = back.at[there]
            number = peers * middle + d
            if d == 0:
                copy = pltpu.make_async_copy(src, dst, recv_o.at[number])
            else:
                copy = pltpu.make_async_remote_copy(
                    src_ref=src,
                    dst_ref=dst,
                    send_sem=send_o.at[number],
                    recv_sem=recv_o.at[number],
                    device_id=peer(q),
                    device_id_type=mesh_id,
                )
            copy.start()
            out_copies.append(copy)
    sent_out = []
    for number, copy in enumerate(out_copies):
        if number in (0, peers):
            copy.wait()
        else:
            copy.wait_recv()
            sent_out.append(copy)
    for j in range(blocks):
        parts = []
        for k in range(fold):
            line = back[:, fold * j + k, :]
            parts.append(
                jnp.concatenate(
                    [line, jnp.zeros((mixed.shape[1] // fold - groups, lanes), jnp.float32)], axis=0
                )
            )
        for b in range(fold):
            mixed[j, pl.ds(b, mixed.shape[1] // fold, stride=fold), :] = gathered(parts, [b] * fold)
    results = []
    for j in range(blocks):
        unpacked[lanes * j : lanes * (j + 1), :] = exact(mixed[j, 0:rows], turn).T
    for x in range(slab):
        at = jnp.where(flip_x, slab - 1 - x, x)
        copy = pltpu.make_async_copy(
            unpacked.at[pl.ds(pl.multiple_of(at * depth, 8), depth)], out_ref.at[0, x], out_sem.at[x]
        )
        copy.start()
        results.append(copy)
    for copy in data_copies[1:] + label_copies[1:] + [mat_copy] + pending + sent_out:
        copy.wait_send()
    for copy in results:
        copy.wait()


def by_rows(data, labels, kernel, offsets):
    tiles = lax.axis_size("tile")
    _, slab, rows, depth = data.shape
    fold = 128 // depth
    tall = -(-rows // (8 * fold)) * 8 * fold
    groups = rows // fold
    cells = slab * tiles
    peers = 2 * tiles
    width = 4
    flat = (slab * depth, rows)
    wide = (2, width, cells, 128)
    dma = pltpu.SemaphoreType.DMA
    taps = kernel.transpose(2, 0, 1)
    result = pl.pallas_call(
        functools.partial(fused, tiles),
        out_shape=jax.ShapeDtypeStruct((1, slab, depth, rows), jnp.float32),
        in_specs=[pl.BlockSpec(memory_space=pl.ANY)] * 4,
        out_specs=pl.BlockSpec(memory_space=pl.ANY),
        scratch_shapes=[
            pltpu.VMEM(flat, jnp.float32),
            pltpu.VMEM(flat, jnp.int32),
            pltpu.VMEM(taps.shape, jnp.float32),
            pltpu.VMEM(offsets.shape, jnp.int32),
            pltpu.VMEM((slab * depth // 128, tall, 128), jnp.float32),
            pltpu.VMEM((groups + 2, slab, 128), jnp.float32),
            pltpu.VMEM((groups + 2, slab, 128), jnp.float32),
            pltpu.VMEM(wide, jnp.float32),
            pltpu.VMEM(wide, jnp.float32),
            pltpu.VMEM((2, depth, 128), jnp.float32),
            pltpu.VMEM(wide, jnp.float32),
            pltpu.VMEM((3,) + wide, jnp.float32),
            pltpu.VMEM((ITERS,) + wide[1:], jnp.float32),
            pltpu.VMEM((ITERS,) + wide[1:], jnp.float32),
            pltpu.VMEM((ITERS - 1, 2, 2, cells, 128), jnp.float32),
            pltpu.VMEM((groups, slab, 128), jnp.float32),
            pltpu.VMEM(flat, jnp.float32),
            dma((2 * slab + 2,)),
            dma((peers,)),
            dma((peers,)),
            dma((peers,)),
            dma((peers,)),
            dma(()),
            dma(()),
            dma((ITERS, 3)),
            dma((ITERS, 3)),
            dma((ITERS - 1, 2)),
            dma((ITERS - 1, 2)),
            dma((peers + tiles,)),
            dma((peers + tiles,)),
            dma((slab,)),
        ],
        compiler_params=pltpu.CompilerParams(collective_id=0, has_side_effects=True),
    )(data.transpose(0, 1, 3, 2), labels.transpose(0, 1, 3, 2), taps, offsets)
    return result.transpose(0, 1, 3, 2)


def fits(data, tiles, views):
    _, slab, rows, depth = data.shape
    return (
        views == 4
        and depth * 4 == 128
        and slab * tiles == depth
        and slab % 8 == 0
        and rows == 12 * tiles
    )


def program(data, labels, kernel, offsets):
    if fits(data, lax.axis_size("tile"), lax.axis_size("view")):
        return by_rows(data, labels, kernel, offsets)
    return on_device(data, labels, kernel, offsets)


def solution(mesh):
    placed = (
        P(("parts", "view"), "tile", None, None),
        P(("parts", "view"), "tile", None, None),
        P("view", None, None),
        P("view", None),
    )
    return jax.shard_map(
        program,
        mesh=mesh,
        in_specs=placed,
        out_specs=P(("parts", "view"), "tile", None, None),
        check_vma=False,
    )
```

```python
import functools

import jax
import jax.numpy as jnp
from jax import lax
from jax.experimental import pallas as pl
from jax.experimental.pallas import tpu as pltpu
from jax.sharding import PartitionSpec as P

ITERS = 2
SWEEPS = 4


WEAK = 0.2
TAU = 0.15


def extended(cells, sides, width):
    for axis, dim in sides:
        count = lax.axis_size(axis)
        ends = count - 1
        head = lax.slice_in_dim(cells, 0, width, axis=dim)
        tail = lax.slice_in_dim(cells, cells.shape[dim] - width, cells.shape[dim], axis=dim)
        cells = jnp.concatenate(
            [
                lax.ppermute(tail, axis, [(i, (i + 1) % count) for i in range(ends)]),
                cells,
                lax.ppermute(head, axis, [((i + 1) % count, i) for i in range(ends)]),
            ],
            axis=dim,
        )
    return cells


def swapped(block, axis, stride):
    count = lax.axis_size(axis)
    route = []
    for low in range(count):
        high = low | 1 << stride
        if high != low and high < count:
            route += [(low, high), (high, low)]
    return lax.ppermute(block, axis, route)


def band(kernel, offsets):
    depth_cells = kernel.shape[0]
    taps = jnp.arange(kernel.shape[1], dtype=jnp.int32) - 4
    depth = jnp.arange(depth_cells, dtype=jnp.int32)
    index = jnp.clip(depth[:, None] + taps[None, :] + offsets[:, None], 0, depth_cells - 1)
    weight = kernel / jnp.sum(kernel, axis=1, keepdims=True)
    return (index, weight)


def axis_term(field, region, axis):
    count = field.shape[axis]
    upper = lax.slice_in_dim(field, 1, count, axis=axis)
    lower = lax.slice_in_dim(field, 0, count - 1, axis=axis)
    same = jnp.where(
        lax.slice_in_dim(region, 1, count, axis=axis)
        == lax.slice_in_dim(region, 0, count - 1, axis=axis),
        1.0,
        WEAK,
    )
    flux = same * (upper - lower)
    after = [(0, 0)] * 3
    before = [(0, 0)] * 3
    after[axis] = (0, 1)
    before[axis] = (1, 0)
    return jnp.pad(flux, after) - jnp.pad(flux, before)


def sweep_rows(field, region, first_row, total_rows):
    extent = field.shape[0]
    global_rows = first_row + jnp.arange(extent, dtype=jnp.int32)
    inside = ((global_rows >= 0) & (global_rows < total_rows)).astype(field.dtype)[:, None, None]
    same = jnp.where(region[1:] == region[:-1], 1.0, WEAK) * inside[1:] * inside[:-1]
    flux = same * (field[1:] - field[:-1])
    inner = field[1:-1]
    inner_labels = region[1:-1]
    total = (
        flux[1:] - flux[:-1] + axis_term(inner, inner_labels, 1) + axis_term(inner, inner_labels, 2)
    )
    return inner + TAU * total


def regroup(received, tiles):
    slab, rows, depth_cells = received.shape
    blocks = received.reshape(slab, rows, tiles, depth_cells // tiles)
    return blocks.transpose(3, 1, 2, 0).reshape(depth_cells // tiles, rows, depth_cells)


def on_device(data, labels, kernel, offsets):
    recorded = data[0]
    region = labels[0]
    index, weight = band(kernel[0], offsets[0])
    tiles = lax.axis_size("tile")
    slab, rows, depth_cells = recorded.shape
    total_rows = slab * tiles
    start = lax.axis_index("tile") * slab
    parity = lax.axis_index("view") % 2
    columns = jnp.arange(depth_cells, dtype=jnp.int32)
    matrix = jnp.sum(weight[:, :, None] * (index[:, :, None] == columns[None, None, :]), axis=1)
    label_ext = extended(region, (("tile", 0),), 4)
    current = recorded
    for step in range(ITERS):
        forward_flat = jnp.dot(
            current.reshape(-1, depth_cells), matrix.T, precision=lax.Precision.HIGHEST
        )
        field = recorded / forward_flat.reshape(current.shape)
        flat = jnp.dot(field.reshape(-1, depth_cells), matrix, precision=lax.Precision.HIGHEST)
        correction = flat.reshape(field.shape)
        turned = correction
        for repeat in range(2):
            turned = regroup(
                lax.all_to_all(
                    jnp.flip(turned, 2), "tile", split_axis=2, concat_axis=2, tiled=True
                ),
                tiles,
            )
        turned = swapped(turned, "view", 1)
        paired = jnp.sqrt(correction * turned)
        outgoing = jnp.where(parity == 0, jnp.flip(paired, 2), paired)
        rotated = regroup(
            lax.all_to_all(outgoing, "tile", split_axis=2, concat_axis=2, tiled=True), tiles
        )
        rotated = jnp.where(parity == 1, jnp.flip(rotated, 2), rotated)
        partner = swapped(rotated, "view", 0)
        current = current * jnp.sqrt(paired * partner)
        widened = extended(current, (("tile", 0),), 4)
        for sweep in range(SWEEPS):
            extent = widened.shape[0]
            widened = sweep_rows(
                widened, label_ext[sweep : sweep + extent], start - 4 + sweep, total_rows
            )
        current = widened
    return current[None]


def gathered(parts, b_of, slot, depth):
    fold = len(parts)
    lanes = parts[0].shape[1]
    total = None
    for k in range(fold):
        amount = (depth * (k - b_of[k])) % lanes
        piece = pltpu.roll(parts[k], amount, 1) if amount else parts[k]
        total = piece if total is None else jnp.where(slot == k, piece, total)
    return total


def turning(lanes, depth, flip_z):
    row_ids = lax.broadcasted_iota(jnp.int32, (lanes, lanes), 0)
    lane_ids = lax.broadcasted_iota(jnp.int32, (lanes, lanes), 1)
    same_block = (row_ids // depth) == (lane_ids // depth)
    aim = jnp.where(flip_z, depth - 1 - lane_ids % depth, lane_ids % depth)
    return same_block, jnp.where(same_block & (row_ids % depth == aim), 1.0, 0.0).astype(jnp.float32)


def exact(a, b):
    return jnp.dot(a, b, precision=lax.Precision.HIGHEST, preferred_element_type=jnp.float32)


def product(a, b, contract):
    return lax.dot_general(a, b, (contract, ((), ())), preferred_element_type=jnp.float32)


def halves(a):
    high = a.astype(jnp.bfloat16)
    return high, (a - high.astype(jnp.float32)).astype(jnp.bfloat16)


def permuted(a, turn):
    high, low = halves(a)
    turn = turn.astype(jnp.bfloat16)
    return product(high, turn, ((1,), (0,))) + product(low, turn, ((1,), (0,)))


def blurred(a, matrix, contract):
    high, low = halves(a)
    return product(high, matrix[0], contract) + (
        product(low, matrix[0], contract) + product(high, matrix[1], contract)
    )


def laid_out(back_ref, out_ref, back, mixed, unpacked, in_sem, out_sem):
    copy = pltpu.make_async_copy(back_ref, back, in_sem)
    copy.start()
    slab, depth, rows = out_ref.shape[1:]
    groups, _, lanes = back.shape
    fold = lanes // depth
    blocks = mixed.shape[0]
    view = lax.axis_index("view")
    flip_x = (view == 1) | (view == 2)
    _, turn = turning(lanes, depth, view >= 2)
    slot = lax.broadcasted_iota(jnp.int32, (mixed.shape[1] // fold, lanes), 1) // depth
    copy.wait()
    results = []
    for j in range(blocks):
        parts = []
        for k in range(fold):
            line = back[:, fold * j + k, :]
            parts.append(
                jnp.concatenate(
                    [line, jnp.zeros((mixed.shape[1] // fold - groups, lanes), jnp.float32)], axis=0
                )
            )
        for b in range(fold):
            mixed[j, pl.ds(b, mixed.shape[1] // fold, stride=fold), :] = gathered(
                parts, [b] * fold, slot, depth
            )
        unpacked[lanes * j : lanes * (j + 1), :] = permuted(mixed[j, 0:rows], turn).T
        for k in range(fold):
            x = fold * j + k
            copy = pltpu.make_async_copy(
                unpacked.at[pl.ds(x * depth, depth)],
                out_ref.at[0, jnp.where(flip_x, slab - 1 - x, x)],
                out_sem.at[x],
            )
            copy.start()
            results.append(copy)
    for copy in results:
        copy.wait()


def fused(tiles, data_ref, labels_ref, taps_ref, shift_ref, back, raw, raw_labels, taps_buf, shift_buf, mixed, packed, packed_labels, held, held_labels, mats, est, coef, outgoing, incoming, halo, in_sem, send, recv, send_l, recv_l, send_m, recv_m, send_p, recv_p, send_h, recv_h, send_o, recv_o):
    mesh_id = pl.DeviceIdType.MESH
    slab, depth, rows = data_ref.shape[1:]
    lanes = packed.shape[2]
    fold = lanes // depth
    groups = rows // fold
    per_tile = groups // tiles
    width = held.shape[1]
    cells = held.shape[2]
    peers = 2 * tiles
    view = lax.axis_index("view")
    tile = lax.axis_index("tile")
    part = lax.axis_index("parts")
    half = view // 2
    core = view % 2
    me = half * tiles + tile
    role = (half + tile) % 2
    flip_x = (view == 1) | (view == 2)
    flip_z = view >= 2

    def peer(q):
        return (part, 2 * (q // tiles) + core, q % tiles)

    copies_in = []
    for source, target, base in ((data_ref, raw, 0), (labels_ref, raw_labels, slab)):
        for x in range(slab):
            at = jnp.where(flip_x, slab - 1 - x, x)
            copies_in.append(
                pltpu.make_async_copy(
                    source.at[0, x],
                    target.at[pl.ds(pl.multiple_of(at * depth, 8), depth)],
                    in_sem.at[base + x],
                )
            )
    copies_in.append(pltpu.make_async_copy(taps_ref, taps_buf, in_sem.at[2 * slab]))
    copies_in.append(pltpu.make_async_copy(shift_ref, shift_buf, in_sem.at[2 * slab + 1]))
    for copy in copies_in:
        copy.start()

    barrier = pltpu.get_barrier_semaphore()
    across = (part, 2 * half + 1 - core, tile)
    for d in range(1, peers):
        pl.semaphore_signal(barrier, inc=1, device_id=peer((me + d) % peers), device_id_type=mesh_id)
    pl.semaphore_signal(barrier, inc=1, device_id=across, device_id_type=mesh_id)

    same_block, turn = turning(lanes, depth, flip_z)
    slot = lax.broadcasted_iota(jnp.int32, (mixed.shape[1] // fold, lanes), 1) // depth
    blocks = slab * depth // lanes

    def pack(source, target, fill, turner):
        edge = jnp.full((1, slab, lanes), fill, jnp.float32)
        target[0:1] = edge
        target[groups + 1 : groups + 2] = edge
        for j in range(blocks):
            mixed[j, 0:rows] = turner(source[lanes * j : lanes * (j + 1), :])
        for j in range(blocks):
            parts = [
                mixed[j, pl.ds(b, mixed.shape[1] // fold, stride=fold), :] for b in range(fold)
            ]
            for k in range(fold):
                line = gathered(parts, [k] * fold, slot, depth)
                target[1 : groups + 1, fold * j + k, :] = line[:groups]

    def turned_labels(block):
        block = block.astype(jnp.float32).T.astype(jnp.bfloat16)
        return product(block, turn.astype(jnp.bfloat16), ((1,), (0,)))

    spot = pl.ds(pl.multiple_of(jnp.where(flip_x, tiles - 1 - tile, tile) * slab, 8), slab)

    def scatter(source, target, send_sem, recv_sem):
        copies = []
        for d in range(peers):
            q = (me + d) % peers
            src = source.at[pl.ds(per_tile * (q % tiles) + (q // tiles + q % tiles) % 2, width)]
            dst = target.at[half, :, spot, :]
            if d == 0:
                copy = pltpu.make_async_copy(src, dst, recv_sem.at[0])
            else:
                copy = pltpu.make_async_remote_copy(
                    src_ref=src,
                    dst_ref=dst,
                    send_sem=send_sem.at[d],
                    recv_sem=recv_sem.at[d],
                    device_id=peer(q),
                    device_id_type=mesh_id,
                )
            copy.start()
            copies.append(copy)
        return copies

    def landed(copies):
        copies[0].wait()
        for copy in copies[1:]:
            copy.wait_recv()

    for x in range(slab):
        copies_in[x].wait()
    pack(raw, packed, 1.0, lambda v: permuted(v.T, turn))
    pl.semaphore_wait(barrier, peers)
    data_copies = scatter(packed, held, send, recv)

    copies_in[2 * slab].wait()
    copies_in[2 * slab + 1].wait()
    count = taps_buf.shape[0]
    taps = [jnp.concatenate([taps_buf[k]] * fold, axis=1) for k in range(count)]
    scale = taps[0]
    for k in range(1, count):
        scale = scale + taps[k]
    shift = jnp.concatenate([shift_buf[...]] * fold, axis=1)
    level = lax.broadcasted_iota(jnp.int32, (1, lanes), 1) % depth
    strip_row = lax.broadcasted_iota(jnp.int32, (depth, lanes), 0)
    strip_aim = jnp.where(flip_z, depth - 1 - strip_row, strip_row)
    strip = jnp.zeros((depth, lanes), jnp.float32)
    for k in range(count):
        index = jnp.clip(level + (k - 4) + shift, 0, depth - 1)
        strip = strip + jnp.where(index == strip_aim, taps[k] / scale, 0.0)
    strip = exact(strip, turn)
    mats[pl.ds(half, 1)] = strip[None]
    mat_copy = pltpu.make_async_remote_copy(
        src_ref=mats.at[half],
        dst_ref=mats.at[half],
        send_sem=send_m,
        recv_sem=recv_m,
        device_id=(part, 2 * (1 - half) + core, tile),
        device_id_type=mesh_id,
    )
    mat_copy.start()

    for x in range(slab):
        copies_in[slab + x].wait()
    pack(raw_labels, packed_labels, 0.0, turned_labels)
    label_copies = scatter(packed_labels, held_labels, send_l, recv_l)

    lane = lax.broadcasted_iota(jnp.int32, (cells, lanes), 1)
    sub = lax.broadcasted_iota(jnp.int32, (cells, lanes), 0)
    first = per_tile * tile - 1 + role
    last_lane = lane < lanes - depth
    first_lane = lane < depth

    def ahead_y(fields, g):
        return jnp.where(
            last_lane,
            pltpu.roll(fields[g], lanes - depth, 1),
            pltpu.roll(fields[(g + 1) % width], lanes - depth, 1),
        )

    def behind_y(fields, g):
        return jnp.where(
            first_lane,
            pltpu.roll(fields[g - 1], depth, 1),
            pltpu.roll(fields[g], depth, 1),
        )

    def transposed(p, chosen):
        flipped = p.T
        result = []
        for g in chosen:
            piece = flipped[0:depth]
            if g:
                piece = pltpu.roll(piece, (lanes - depth * g) % lanes, 1)
            for b in range(1, fold):
                part_b = flipped[depth * b : depth * (b + 1)]
                amount = (depth * (b - g)) % lanes
                if amount:
                    part_b = pltpu.roll(part_b, amount, 1)
                piece = jnp.where(lane // depth == b, part_b, piece)
            result.append(piece)
        return result

    landed(data_copies)
    mat_copy.wait_recv()
    blurs = [
        halves(jnp.where(same_block, jnp.concatenate([mats[s]] * fold, axis=0), 0.0))
        for s in range(2)
    ]

    def paired_of(step, chosen):
        corrections = []
        for s in range(2):
            recorded = jnp.concatenate([held[s, g] for g in chosen], axis=0)
            if step == 0:
                current = recorded
            else:
                current = jnp.concatenate([est[s, g] for g in chosen], axis=0)
            ratio = recorded / blurred(current, blurs[s], ((1,), (0,)))
            corrections.append(blurred(ratio, blurs[s], ((1,), (1,))))
        return jnp.sqrt(corrections[0] * corrections[1])

    def swapped_over(step, number, begin, size):
        copy = pltpu.make_async_remote_copy(
            src_ref=outgoing.at[step, pl.ds(begin, size)],
            dst_ref=incoming.at[step, pl.ds(begin, size)],
            send_sem=send_p.at[step, number],
            recv_sem=recv_p.at[step, number],
            device_id=across,
            device_id_type=mesh_id,
        )
        copy.start()
        pending.append(copy)
        return copy

    far = tile + 2 * role - 1
    exists = (far >= 0) & (far < tiles)

    def leaving(s, d, middle, relation):
        t = (tile + d) % tiles
        place = jnp.where(core == 1 - s, tiles - 1 - t, t)
        here = 2 - role if middle else 1 + role
        there = per_tile * tile + (1 if middle else 2 * role)
        src = est.at[s, here, pl.ds(pl.multiple_of(place * slab, 8), slab), :]
        if relation is None:
            return pltpu.make_async_copy(src, back.at[there], recv_o.at[0, middle])
        return pltpu.make_async_remote_copy(
            src_ref=src,
            dst_ref=back.at[there],
            send_sem=send_o.at[s, 2 * d + middle],
            recv_sem=recv_o.at[relation, 2 * d + middle],
            device_id=(part, 2 * s + core, t),
            device_id_type=mesh_id,
        )

    def arrived(d, middle, relation):
        origin = (tile + tiles - d) % tiles
        its_role = (half + relation + origin) % 2
        there = per_tile * origin + (1 if middle else 2 * its_role)
        pltpu.make_async_remote_copy(
            src_ref=back.at[there],
            dst_ref=back.at[there],
            send_sem=send_o.at[0, 2 * d + middle],
            recv_sem=recv_o.at[relation, 2 * d + middle],
            device_id=across,
            device_id_type=mesh_id,
        ).wait_recv()

    def send_back(s):
        for d in range(1, tiles):
            leaving(s, d, 0, (s + half) % 2).start()

        @pl.when(half == 1 - s)
        def _():
            leaving(s, 0, 0, 1).start()

        @pl.when(half == s)
        def _():
            for d in range(1, tiles):
                leaving(s, d, 1, 0).start()
            for middle in range(2):
                leaving(s, 0, middle, None).start()

    def sent_back(s):
        for d in range(1, tiles):
            leaving(s, d, 0, (s + half) % 2).wait_send()

        @pl.when(half == 1 - s)
        def _():
            leaving(s, 0, 0, 1).wait_send()

        @pl.when(half == s)
        def _():
            for d in range(1, tiles):
                leaving(s, d, 1, 0).wait_send()
            for middle in range(2):
                leaving(s, 0, middle, None).wait()

    pending = []
    ready = {}
    for step in range(ITERS):
        if step == 0:
            whole = paired_of(0, range(width))
            for g, piece in enumerate(transposed(whole, range(width))):
                outgoing[step, g] = piece
                ready[g] = whole[cells * g : cells * (g + 1)]
            swaps = [swapped_over(step, 0, 0, width)]
        else:
            inner = range(1, width - 1)
            outer = (0, width - 1)
            swaps = []
            for number, chosen in enumerate((inner, outer)):
                if number:
                    near = (width - 1) * (1 - role)
                    for s in range(2):
                        near_copies[s].wait()
                        est[s, pl.ds(near, 1)] = halo[step - 1, 1 - role, s][None]

                    @pl.when(exists)
                    def _():
                        for s in range(2):
                            far_copies[s].wait()
                            est[s, pl.ds((width - 1) * role, 1)] = halo[step - 1, role, s][None]

                part_p = paired_of(step, chosen)
                turned_p = transposed(jnp.concatenate([part_p, part_p], axis=0), range(len(chosen)))
                for k, g in enumerate(chosen):
                    outgoing[step, g] = turned_p[k]
                    ready[g] = part_p[cells * k : cells * (k + 1)]
                if number:
                    swaps += [swapped_over(step, 1 + k, g, 1) for k, g in enumerate(chosen)]
                else:
                    swaps.append(swapped_over(step, 0, 1, width - 2))
        if step == 0:
            landed(label_copies)
            for s in range(2):
                regions = [held_labels[s, g] for g in range(width)]
                for g in range(width):
                    mine = regions[g]
                    strong, weak = TAU, TAU * WEAK
                    e_x = jnp.where(pltpu.roll(mine, cells - 1, 0) == mine, strong, weak)
                    coef[0, s, g] = jnp.where(sub == cells - 1, 0.0, e_x)
                    e_z = jnp.where(pltpu.roll(mine, lanes - 1, 1) == mine, strong, weak)
                    coef[1, s, g] = jnp.where(lane % depth == depth - 1, 0.0, e_z)
                    e_y = jnp.where(ahead_y(regions, g) == mine, strong, weak)
                    y = fold * (first + g) + lane // depth
                    coef[2, s, g] = jnp.where((y >= 0) & (y < rows - 1), e_y, 0.0)
        for swap in swaps:
            swap.wait_recv()
        joined = [jnp.sqrt(ready[g] * incoming[step, g]) for g in range(width)]
        last = step == ITERS - 1
        near_copies, far_copies = [], []
        for s in range(2):
            base = held if step == 0 else est
            fields = [base[s, g] * joined[g] for g in range(width)]
            for sweep in range(SWEEPS):
                kept = range(1, width - 1) if sweep == SWEEPS - 1 else range(width)
                flux_y = {
                    g: coef[2, s, g] * (ahead_y(fields, g) - fields[g])
                    for g in range(kept[0] - 1 if kept[0] else 0, kept[-1] + 1)
                }
                if kept[0] == 0:
                    flux_y[-1] = flux_y[width - 1]
                fresh = list(fields)
                for g in kept:
                    f = fields[g]
                    flux_x = coef[0, s, g] * (pltpu.roll(f, cells - 1, 0) - f)
                    flux_z = coef[1, s, g] * (pltpu.roll(f, lanes - 1, 1) - f)
                    total = (
                        (flux_x - pltpu.roll(flux_x, 1, 0))
                        + (flux_y[g] - behind_y(flux_y, g))
                        + (flux_z - pltpu.roll(flux_z, 1, 1))
                    )
                    fresh[g] = f + total
                fields = fresh
            for g in range(width):
                est[s, g] = fields[g]
            if last:
                send_back(s)
                continue

            def shifted(number, side, x_of, target):
                return pltpu.make_async_remote_copy(
                    src_ref=est.at[s, 1 + role],
                    dst_ref=halo.at[step, side, s],
                    send_sem=send_h.at[step, number, s],
                    recv_sem=recv_h.at[step, number, s],
                    device_id=(part, 2 * x_of + core, target),
                    device_id_type=mesh_id,
                )

            near_copies.append(shifted(0, role, 1 - half, tile))
            far_copies.append(shifted(1, 1 - role, half, jnp.clip(far, 0, tiles - 1)))
            near_copies[s].start()

            @pl.when(exists)
            def _():
                far_copies[s].start()

    for d in range(tiles):
        arrived(d, 0, 1)
        if d:
            arrived(d, 0, 0)
            arrived(d, 1, 0)
    for s in range(2):
        sent_back(s)
    for copy in data_copies[1:] + label_copies[1:] + [mat_copy] + pending:
        copy.wait_send()


def by_rows(data, labels, kernel, offsets):
    tiles = lax.axis_size("tile")
    _, slab, rows, depth = data.shape
    fold = 128 // depth
    tall = -(-rows // (8 * fold)) * 8 * fold
    groups = rows // fold
    cells = slab * tiles
    peers = 2 * tiles
    width = 4
    flat = (slab * depth, rows)
    wide = (2, width, cells, 128)
    dma = pltpu.SemaphoreType.DMA
    taps = kernel.transpose(2, 0, 1)
    back = pl.pallas_call(
        functools.partial(fused, tiles),
        out_shape=jax.ShapeDtypeStruct((groups, slab, 128), jnp.float32),
        in_specs=[pl.BlockSpec(memory_space=pltpu.HBM)] * 4,
        out_specs=pl.BlockSpec(memory_space=pl.ANY),
        scratch_shapes=[
            pltpu.VMEM(flat, jnp.float32),
            pltpu.VMEM(flat, jnp.int32),
            pltpu.VMEM(taps.shape, jnp.float32),
            pltpu.VMEM(offsets.shape, jnp.int32),
            pltpu.VMEM((slab * depth // 128, tall, 128), jnp.float32),
            pltpu.VMEM((groups + 2, slab, 128), jnp.float32),
            pltpu.VMEM((groups + 2, slab, 128), jnp.float32),
            pltpu.VMEM(wide, jnp.float32),
            pltpu.VMEM(wide, jnp.float32),
            pltpu.VMEM((2, depth, 128), jnp.float32),
            pltpu.VMEM(wide, jnp.float32),
            pltpu.VMEM((3,) + wide, jnp.float32),
            pltpu.VMEM((ITERS,) + wide[1:], jnp.float32),
            pltpu.VMEM((ITERS,) + wide[1:], jnp.float32),
            pltpu.VMEM((ITERS - 1, 2, 2, cells, 128), jnp.float32),
            dma((2 * slab + 2,)),
            dma((peers,)),
            dma((peers,)),
            dma((peers,)),
            dma((peers,)),
            dma(()),
            dma(()),
            dma((ITERS, 3)),
            dma((ITERS, 3)),
            dma((ITERS - 1, 2, 2)),
            dma((ITERS - 1, 2, 2)),
            dma((2, peers)),
            dma((2, peers)),
        ],
        compiler_params=pltpu.CompilerParams(
            collective_id=0, has_side_effects=True
        ),
    )(data.transpose(0, 1, 3, 2), labels.transpose(0, 1, 3, 2), taps, offsets)
    result = pl.pallas_call(
        laid_out,
        out_shape=jax.ShapeDtypeStruct((1, slab, depth, rows), jnp.float32),
        in_specs=[pl.BlockSpec(memory_space=pl.ANY)],
        out_specs=pl.BlockSpec(memory_space=pltpu.HBM),
        scratch_shapes=[
            pltpu.VMEM((groups, slab, 128), jnp.float32),
            pltpu.VMEM((slab * depth // 128, tall, 128), jnp.float32),
            pltpu.VMEM(flat, jnp.float32),
            dma(()),
            dma((slab,)),
        ],
    )(back)
    return result.transpose(0, 1, 3, 2)


def fits(data, tiles, views):
    _, slab, rows, depth = data.shape
    return (
        views == 4
        and depth * 4 == 128
        and slab * tiles == depth
        and slab % 8 == 0
        and rows == 12 * tiles
    )


def program(data, labels, kernel, offsets):
    if fits(data, lax.axis_size("tile"), lax.axis_size("view")):
        return by_rows(data, labels, kernel, offsets)
    return on_device(data, labels, kernel, offsets)


def solution(mesh):
    placed = (
        P(("parts", "view"), "tile", None, None),
        P(("parts", "view"), "tile", None, None),
        P("view", None, None),
        P("view", None),
    )
    return jax.shard_map(
        program,
        mesh=mesh,
        in_specs=placed,
        out_specs=P(("parts", "view"), "tile", None, None),
        check_vma=False,
    )
```
